8 devices in a mesh: dp: 1 (over z), ep: 8 (over y, x, core).
Axes of the slice: x: 2, y: 2, z: 1, core: 2. Of those that a mesh axis runs over, the one named last changes fastest.
Arguments:
- hidden: bfloat16 [16384, 2048], P(('dp', 'ep'))
- w_router: bfloat16 [2048, 64], replicated
- w_gate: bfloat16 [64, 2048, 1408], P('ep')
- w_up: bfloat16 [64, 2048, 1408], P('ep')
- w_down: bfloat16 [64, 1408, 2048], P('ep')
- shared_gate: bfloat16 [2048, 2816], replicated
- shared_up: bfloat16 [2048, 2816], replicated
- shared_down: bfloat16 [2816, 2048], replicated
- top_idx: int32 [16384, 6], P(('dp', 'ep'))
- keep_mask: int32 [16384, 6], P(('dp', 'ep'))
Outputs:
- output: bfloat16 [16384, 2048], P(('dp', 'ep'))
All inputs are finite; a program needn't handle non-finite values.
Results may differ from the reference program's by a relative error of at most 0.00689379.
Values are sent between devices in bfloat16 or wider.
A program may use at most 1 GiB of HBM per device.

```python
import math
import jax
import jax.numpy as jnp
from jax import lax

HIDDEN = 2048
EXPERTS = 64
EXPERT_FF = 1408
SHARED_FF = 2816
TOP_K = 6
DEV_LIMIT = 6
TOKENS = 2048
GROUP_SIZE = 8
CAPACITY = 384

ROUTE_SCALE = 16.0
PER_DEVICE = EXPERTS // GROUP_SIZE
PART_TOKENS = GROUP_SIZE * TOKENS
ROUTED_GAIN = EXPERTS / (ROUTE_SCALE * math.sqrt(TOP_K))


def draw_routing(route_key):
    k_noise, k_dev, k_exp, k_hot = jax.random.split(route_key, 4)
    expert_ids = jnp.arange(EXPERTS, dtype=jnp.int32)
    noise_int = jax.random.randint(k_noise, (PART_TOKENS, EXPERTS), 0, 256, dtype=jnp.int32)
    dev_bias = jax.random.randint(k_dev, (GROUP_SIZE,), 0, 128, dtype=jnp.int32)
    exp_bias = jax.random.randint(k_exp, (EXPERTS,), 0, 64, dtype=jnp.int32)
    hot_expert = jax.random.randint(k_hot, (), 0, EXPERTS, dtype=jnp.int32)
    bias_all = exp_bias + jnp.repeat(dev_bias, PER_DEVICE) + jnp.where(expert_ids == hot_expert, 1024, 0)
    pair_score = (noise_int + bias_all[None, :]) * EXPERTS + expert_ids[None, :]
    dev_score = jnp.max(pair_score.reshape(PART_TOKENS, GROUP_SIZE, PER_DEVICE), axis=2)
    top_dev = lax.top_k(dev_score, DEV_LIMIT)[1]
    chosen = jnp.any(top_dev[:, :, None] == jnp.arange(GROUP_SIZE, dtype=jnp.int32)[None, None, :], axis=1)
    masked = jnp.where(jnp.repeat(chosen, PER_DEVICE, axis=1), pair_score, -1)
    top_idx = lax.top_k(masked, TOP_K)[1].astype(jnp.int32)

    def rank_pairs(src_pairs):
        onehot = (src_pairs[:, None] == expert_ids[None, :]).astype(jnp.int32)
        return jnp.sum((jnp.cumsum(onehot, axis=0) - 1) * onehot, axis=1)

    pair_rank = lax.map(rank_pairs, top_idx.reshape(GROUP_SIZE, TOKENS * TOP_K))
    keep_mask = (pair_rank < CAPACITY).astype(jnp.int32).reshape(PART_TOKENS, TOP_K)
    return top_idx, keep_mask


def draw_bank(bank_key, mat_shape, std_scale):
    key_list = jax.random.split(bank_key, EXPERTS)
    return lax.map(lambda one_key: (jax.random.normal(one_key, mat_shape, jnp.float32) * std_scale).astype(jnp.bfloat16), key_list)


def draw_matrix(mat_key, mat_shape, std_scale):
    return (jax.random.normal(mat_key, mat_shape, jnp.float32) * std_scale).astype(jnp.bfloat16)


def setup_inputs(seed: int = 0, part: int = 0) -> dict:
    root_key = jax.random.key(seed)
    part_key = jax.random.fold_in(root_key, part)
    k_hidden, k_route = jax.random.split(part_key, 2)
    k_router, k_gate, k_up, k_down, k_sgate, k_sup, k_sdown = jax.random.split(root_key, 7)
    top_idx, keep_mask = draw_routing(k_route)
    in_scale = HIDDEN ** -0.5
    return {
        "hidden": draw_matrix(k_hidden, (PART_TOKENS, HIDDEN), 1.0),
        "w_router": draw_matrix(k_router, (HIDDEN, EXPERTS), 0.5 * in_scale),
        "w_gate": draw_bank(k_gate, (HIDDEN, EXPERT_FF), in_scale),
        "w_up": draw_bank(k_up, (HIDDEN, EXPERT_FF), in_scale),
        "w_down": draw_bank(k_down, (EXPERT_FF, HIDDEN), ROUTED_GAIN * EXPERT_FF ** -0.5),
        "shared_gate": draw_matrix(k_sgate, (HIDDEN, SHARED_FF), in_scale),
        "shared_up": draw_matrix(k_sup, (HIDDEN, SHARED_FF), in_scale),
        "shared_down": draw_matrix(k_sdown, (SHARED_FF, HIDDEN), SHARED_FF ** -0.5),
        "top_idx": top_idx,
        "keep_mask": keep_mask,
    }


def swiglu(tok_rows, gate_w, up_w, down_w):
    h_gate = jnp.dot(tok_rows, gate_w, preferred_element_type=jnp.float32)
    h_up = jnp.dot(tok_rows, up_w, preferred_element_type=jnp.float32)
    act_rows = (jax.nn.silu(h_gate) * h_up).astype(jnp.bfloat16)
    return jnp.dot(act_rows, down_w, preferred_element_type=jnp.float32)


def reference(hidden, w_router, w_gate, w_up, w_down, shared_gate, shared_up, shared_down, top_idx, keep_mask):
    logits = jnp.dot(hidden, w_router, preferred_element_type=jnp.float32)
    router_prob = jax.nn.softmax(logits, axis=-1)
    gate_vals = ROUTE_SCALE * jnp.take_along_axis(router_prob, top_idx, axis=1) * keep_mask.astype(jnp.float32)
    pair_expert = top_idx.reshape(-1)
    pair_kept = keep_mask.reshape(-1) > 0
    pair_gate = gate_vals.reshape(-1)
    pair_token = jnp.arange(PART_TOKENS * TOP_K, dtype=jnp.int32) // TOP_K
    max_rows = GROUP_SIZE * CAPACITY

    def expert_step(routed_acc, per_expert):
        gate_w, up_w, down_w, expert_id = per_expert
        member = pair_kept & (pair_expert == expert_id)
        pair_slot = jnp.where(member, jnp.cumsum(member.astype(jnp.int32)) - 1, max_rows)
        row_token = jnp.zeros((max_rows,), jnp.int32).at[pair_slot].set(pair_token, mode="drop")
        row_gate = jnp.zeros((max_rows,), jnp.float32).at[pair_slot].set(pair_gate, mode="drop")
        expert_out = swiglu(hidden[row_token], gate_w, up_w, down_w).astype(jnp.bfloat16)
        routed_acc = routed_acc.at[row_token].add(row_gate[:, None] * expert_out.astype(jnp.float32))
        return routed_acc, None

    routed = lax.scan(expert_step, jnp.zeros((PART_TOKENS, HIDDEN), jnp.float32), (w_gate, w_up, w_down, jnp.arange(EXPERTS, dtype=jnp.int32)))[0]
    shared = lax.map(lambda tok_block: swiglu(tok_block, shared_gate, shared_up, shared_down), hidden.reshape(GROUP_SIZE, TOKENS, HIDDEN)).reshape(PART_TOKENS, HIDDEN)
    return (shared + routed).astype(jnp.bfloat16)
```

```python
import functools
import jax
import jax.numpy as jnp
from jax import lax
from jax.experimental import pallas as pl
from jax.experimental.pallas import tpu as pltpu
from jax.sharding import PartitionSpec as P

ROUTE_SCALE = 16.0
CAP = 384
LANES = 128
STRIDE = CAP + 8


def swiglu(tok_rows, gate_w, up_w, down_w):
    h_gate = jnp.dot(tok_rows, gate_w, preferred_element_type=jnp.float32)
    h_up = jnp.dot(tok_rows, up_w, preferred_element_type=jnp.float32)
    act_rows = (jax.nn.silu(h_gate) * h_up).astype(jnp.bfloat16)
    return jnp.dot(act_rows, down_w, preferred_element_type=jnp.float32)


def bank_kernel(tok, gate, cnt, x_hbm, w1a, w3a, w2a, w1b, w3b, w2b, out_hbm,
                x_v, acc, w1v, w3v, w2v, xf, xs, hv, stage, x_sem, w1_sem, w3_sem, w2_sem, out_sem):
    tokens, chunks, _ = x_v.shape
    width = chunks * LANES
    per_dev = w1a.shape[0]
    ff = w1a.shape[2]
    experts = 2 * per_dev

    def copy_w(dst, sem, a, b, e, start):
        @pl.when(e < per_dev)
        def _():
            c = pltpu.make_async_copy(a.at[jnp.minimum(e, per_dev - 1)], dst, sem)
            c.start() if start else c.wait()

        @pl.when(e >= per_dev)
        def _():
            c = pltpu.make_async_copy(b.at[jnp.maximum(e - per_dev, 0)], dst, sem)
            c.start() if start else c.wait()

    def in_copies(e, slot, start):
        copy_w(w1v.at[slot], w1_sem.at[slot], w1a, w1b, e, start)
        copy_w(w3v.at[slot], w3_sem.at[slot], w3a, w3b, e, start)

    xc = pltpu.make_async_copy(x_hbm, x_v, x_sem)
    xc.start()
    in_copies(jnp.int32(0), 0, True)
    copy_w(w2v, w2_sem, w2a, w2b, jnp.int32(0), True)

    rows0 = acc.shape[0]
    zblk = 256

    @pl.loop(0, rows0 // zblk)
    def _(i):
        acc[pl.ds(pl.multiple_of(i * zblk, zblk), zblk), :] = jnp.zeros((zblk, LANES), jnp.float32)

    xc.wait()

    def ffn(m, slot):
        for j in range(chunks):
            xs[0:m, j * LANES:(j + 1) * LANES] = xf[j * STRIDE:j * STRIDE + m, :].astype(jnp.bfloat16)

        def gate_up(c0, cw):
            xv = xs[0:m, :]
            g = jnp.dot(xv, w1v[slot, :, pl.ds(c0, cw)], preferred_element_type=jnp.float32)
            u = jnp.dot(xv, w3v[slot, :, pl.ds(c0, cw)], preferred_element_type=jnp.float32)
            hv[0:m, pl.ds(c0, cw)] = (jax.nn.silu(g) * u).astype(jnp.bfloat16)

        @pl.loop(0, ff // 256)
        def _(c):
            gate_up(pl.multiple_of(c * 256, 256), 256)

        if ff % 256:
            gate_up(ff // 256 * 256, ff % 256)

    def down(m):
        @pl.loop(0, width // 256)
        def _(c):
            o = jnp.dot(hv[0:m, :], w2v[:, pl.ds(pl.multiple_of(c * 256, 256), 256)], preferred_element_type=jnp.float32)
            o = o.astype(jnp.bfloat16).astype(jnp.float32)
            base = pl.multiple_of(c * (2 * STRIDE), 8)
            xf[pl.ds(base, m), :] = o[:, 0:LANES]
            xf[pl.ds(base + STRIDE, m), :] = o[:, LANES:2 * LANES]

    @pl.loop(0, experts)
    def _(e):
        slot = lax.rem(e, 2)
        n = cnt[e]

        @pl.when(e + 1 < experts)
        def _():
            in_copies(e + 1, 1 - slot, True)

        @pl.loop(0, (n + 7) // 8)
        def _(g):
            s0 = pl.multiple_of(g * 8, 8)
            for i in range(8):
                t = jnp.minimum(tok[e, s0 + i], tokens - 1)
                xf[pl.ds(s0 + i, chunks, stride=STRIDE), :] = x_v[t].astype(jnp.float32)

        in_copies(e, slot, False)
        sizes = (128, 256, CAP)
        lo = 0
        for m in sizes:
            @pl.when((n > lo) & (n <= m))
            def _(m=m):
                ffn(m, slot)
            lo = m

        copy_w(w2v, w2_sem, w2a, w2b, e, False)
        lo = 0
        for m in sizes:
            @pl.when((n > lo) & (n <= m))
            def _(m=m):
                down(m)
            lo = m

        @pl.when(e + 1 < experts)
        def _():
            copy_w(w2v, w2_sem, w2a, w2b, e + 1, True)

        @pl.loop(0, (n + 7) // 8)
        def _(g):
            s0 = pl.multiple_of(g * 8, 8)
            for half in range(2):
                sums = []
                for i in range(half * 4, half * 4 + 4):
                    base = pl.multiple_of(tok[e, s0 + i] * chunks, chunks)
                    row = xf[pl.ds(s0 + i, chunks, stride=STRIDE), :]
                    sums.append((base, acc[pl.ds(base, chunks), :] + gate[e, s0 + i] * row))
                for base, val in sums:
                    acc[pl.ds(base, chunks), :] = val

    blk = stage.shape[1]
    n_out = tokens // blk

    @pl.loop(0, n_out)
    def _(i):
        slot = lax.rem(i, 2)
        rows = pl.ds(pl.multiple_of(i * blk, blk), blk)

        @pl.when(i >= 2)
        def _():
            pltpu.make_async_copy(stage.at[slot], out_hbm.at[rows], out_sem.at[slot]).wait()

        for j in range(chunks):
            v = acc[pl.ds(i * (blk * chunks) + j, blk, stride=chunks), :]
            stage[slot, :, j * LANES:(j + 1) * LANES] = v.astype(stage.dtype)
        pltpu.make_async_copy(stage.at[slot], out_hbm.at[rows], out_sem.at[slot]).start()

    for i in range(max(0, n_out - 2), n_out):
        pltpu.make_async_copy(stage.at[i % 2], out_hbm.at[pl.ds(i * blk, blk)], out_sem.at[i % 2]).wait()


def expert_bank(tok, gate, cnt, x3, w_own, w_peer, out_dtype):
    tokens, chunks, _ = x3.shape
    per_dev, width, ff = w_own[0].shape
    blk = 128
    anys = pl.BlockSpec(memory_space=pl.ANY)
    smem = pl.BlockSpec(memory_space=pltpu.SMEM)
    flops = 2 * per_dev * 200 * 6 * width * ff
    return pl.pallas_call(
        bank_kernel,
        out_shape=jax.ShapeDtypeStruct((tokens, width), out_dtype),
        in_specs=[smem] * 3 + [anys] * 7,
        out_specs=anys,
        scratch_shapes=[
            pltpu.VMEM((tokens, chunks, LANES), jnp.bfloat16),
            pltpu.VMEM(((tokens + 16) * chunks, LANES), jnp.float32),
            pltpu.VMEM((2, width, ff), jnp.bfloat16),
            pltpu.VMEM((2, width, ff), jnp.bfloat16),
            pltpu.VMEM((ff, width), jnp.bfloat16),
            pltpu.VMEM((chunks * STRIDE, LANES), jnp.float32),
            pltpu.VMEM((CAP, width), jnp.bfloat16),
            pltpu.VMEM((CAP, ff), jnp.bfloat16),
            pltpu.VMEM((2, blk, width), out_dtype),
            pltpu.SemaphoreType.DMA,
            pltpu.SemaphoreType.DMA((2,)),
            pltpu.SemaphoreType.DMA((2,)),
            pltpu.SemaphoreType.DMA,
            pltpu.SemaphoreType.DMA((2,)),
        ],
        compiler_params=pltpu.CompilerParams(vmem_limit_bytes=66_000_000),
        cost_estimate=pl.CostEstimate(flops=flops, bytes_accessed=6 * per_dev * width * ff * 2, transcendentals=0),
    )(tok, gate, cnt, x3, *w_own, *w_peer)


def solution(mesh):
    groups = mesh.shape["ep"]
    tok_spec = P(("dp", "ep"), None)
    bank_spec = P("ep", None, None)

    def swap(a, s):
        return lax.ppermute(a, "ep", [(i, i ^ s) for i in range(groups)])

    def device_fn(hidden, w_router, w_gate, w_up, w_down, shared_gate, shared_up, shared_down, top_idx, keep_mask):
        tokens, top_k = top_idx.shape
        width = hidden.shape[1]
        experts = w_router.shape[1]
        per_chip = 2 * w_gate.shape[0]
        me = lax.axis_index("ep")
        strides = tuple(range(2, groups, 2))

        x_in = {s: swap(hidden, s) for s in strides}
        w_peer = tuple(swap(w, 1) for w in (w_gate, w_up, w_down))
        w_own = (w_gate, w_up, w_down)

        logits = jnp.dot(hidden, w_router, preferred_element_type=jnp.float32)
        prob = ROUTE_SCALE * jax.nn.softmax(logits, axis=-1)
        kept_id = jnp.where(keep_mask > 0, top_idx, experts)
        member = jnp.any(kept_id[:, :, None] == jnp.arange(experts)[None, None, :], axis=1)
        member_b = member.astype(jnp.bfloat16)
        t_ids = jnp.arange(tokens, dtype=jnp.int32)
        before = (t_ids[:, None] > t_ids[None, :]).astype(jnp.bfloat16)
        rank = jnp.dot(before, member_b, preferred_element_type=jnp.float32).astype(jnp.int32)
        rank = jnp.where(member, rank, -1)
        hit = rank[:, :, None] == jnp.arange(CAP, dtype=jnp.int32)[None, None, :]
        slot_tok = jnp.min(jnp.where(hit, t_ids[:, None, None].astype(jnp.float32), float(tokens)), axis=0)
        slot_gate = jnp.sum(jnp.where(hit, prob[:, :, None], 0.0), axis=0)
        lists = jnp.stack([slot_tok, slot_gate], axis=1)

        def lists_of(dev):
            return lax.dynamic_slice_in_dim(lists, (dev // 2) * per_chip, per_chip, axis=0)

        def run(x2, lst, out_dtype):
            own_first = lax.rem(me, 2) == 0
            half = per_chip // 2
            lst = jnp.where(own_first, lst, jnp.concatenate([lst[half:], lst[:half]], axis=0))
            tok = lst[:, 0].astype(jnp.int32)
            cnt = jnp.sum((tok < tokens).astype(jnp.int32), axis=1)
            x3 = x2.reshape(tokens, width // LANES, LANES)
            return expert_bank(tok, lst[:, 1], cnt, x3, w_own, w_peer, out_dtype)

        l_in = {s: swap(lists_of(me ^ s), s) for s in strides}
        shared = swiglu(hidden, shared_gate, shared_up, shared_down)
        total = shared
        back = []
        for s in strides:
            part = run(x_in[s], l_in[s], jnp.bfloat16)
            back.append(swap(part, s))
        total = total + run(hidden, lists_of(me), jnp.float32)
        for b in back:
            total = total + b.astype(jnp.float32)
        return total.astype(jnp.bfloat16)

    return jax.shard_map(device_fn, mesh=mesh, in_specs=(tok_spec, P(), bank_spec, bank_spec, bank_spec, P(), P(), P(), tok_spec, tok_spec), out_specs=tok_spec, check_vma=False)
```

```python
import jax
import jax.numpy as jnp
from jax import lax
from jax.experimental import pallas as pl
from jax.experimental.pallas import tpu as pltpu
from jax.sharding import PartitionSpec as P

ROUTE_SCALE = 16.0
CAP = 384
LANES = 128
STRIDE = CAP + 8
SIZES = (64, 128, 192, 256, 320, 384)
UNROLL = 16
BATCH = 8


def swiglu(tok_rows, gate_w, up_w, down_w):
    h_gate = jnp.dot(tok_rows, gate_w, preferred_element_type=jnp.float32)
    h_up = jnp.dot(tok_rows, up_w, preferred_element_type=jnp.float32)
    act_rows = (jax.nn.silu(h_gate) * h_up).astype(jnp.bfloat16)
    return jnp.dot(act_rows, down_w, preferred_element_type=jnp.float32)


def bank_kernel(tok, gate, cnt, xa_hbm, xb_hbm, w1a, w3a, w2a, w1b, w3b, w2b, out_hbm,
                x_v, acc, w1v, w3v, w2v, xf, xs, hv, stage, x_sem, w1_sem, w3_sem, w2_sem, out_sem):
    tokens, chunks, _ = x_v.shape
    width = chunks * LANES
    per_dev = w1a.shape[0]
    ff = w1a.shape[2]
    experts = 2 * per_dev

    def copy_w(dst, sem, a, b, e, start):
        @pl.when((e < per_dev) & (cnt[e] > 0))
        def _():
            c = pltpu.make_async_copy(a.at[jnp.minimum(e, per_dev - 1)], dst, sem)
            c.start() if start else c.wait()

        @pl.when((e >= per_dev) & (cnt[e] > 0))
        def _():
            c = pltpu.make_async_copy(b.at[jnp.maximum(e - per_dev, 0)], dst, sem)
            c.start() if start else c.wait()

    def in_copies(e, slot, start):
        copy_w(w1v.at[slot], w1_sem.at[slot], w1a, w1b, e, start)
        copy_w(w3v.at[slot], w3_sem.at[slot], w3a, w3b, e, start)

    half = tokens // 2
    x_copies = [pltpu.make_async_copy(src, x_v.at[pl.ds(i * half, half)], x_sem.at[i]) for i, src in enumerate((xa_hbm, xb_hbm))]
    for c in x_copies:
        c.start()
    in_copies(jnp.int32(0), 0, True)
    copy_w(w2v, w2_sem, w2a, w2b, jnp.int32(0), True)

    rows0 = acc.shape[0]
    zblk = 256

    @pl.loop(0, rows0 // zblk)
    def _(i):
        acc[pl.ds(pl.multiple_of(i * zblk, zblk), zblk), :] = jnp.zeros((zblk, LANES), jnp.float32)

    for c in x_copies:
        c.wait()

    def ffn(m, slot):
        for j in range(chunks):
            xs[0:m, j * LANES:(j + 1) * LANES] = xf[j * STRIDE:j * STRIDE + m, :].astype(jnp.bfloat16)

        def gate_up(c0, cw):
            xv = xs[0:m, :]
            g = jnp.dot(xv, w1v[slot, :, c0:c0 + cw], preferred_element_type=jnp.float32)
            u = jnp.dot(xv, w3v[slot, :, c0:c0 + cw], preferred_element_type=jnp.float32)
            hv[0:m, c0:c0 + cw] = (jax.nn.silu(g) * u).astype(jnp.bfloat16)

        for c0 in range(0, ff, 768):
            gate_up(c0, min(768, ff - c0))

    def down(m):
        cols = 1024

        @pl.loop(0, width // cols)
        def _(c):
            o = jnp.dot(hv[0:m, :], w2v[:, pl.ds(pl.multiple_of(c * cols, cols), cols)], preferred_element_type=jnp.float32)
            o = o.astype(jnp.bfloat16).astype(jnp.float32)
            base = pl.multiple_of(c * (cols // LANES * STRIDE), 8)
            for j in range(cols // LANES):
                xf[pl.ds(base + j * STRIDE, m), :] = o[:, j * LANES:(j + 1) * LANES]

    @pl.loop(0, experts)
    def _(e):
        slot = lax.rem(e, 2)
        n = cnt[e]

        @pl.when(e + 1 < experts)
        def _():
            in_copies(e + 1, 1 - slot, True)

        @pl.loop(0, (n + UNROLL - 1) // UNROLL)
        def _(g):
            s0 = pl.multiple_of(g * UNROLL, UNROLL)
            for i in range(UNROLL):
                t = jnp.minimum(tok[e, s0 + i], tokens - 1)
                xf[pl.ds(s0 + i, chunks, stride=STRIDE), :] = x_v[t].astype(jnp.float32)

        in_copies(e, slot, False)
        lo = 0
        for m in SIZES:
            @pl.when((n > lo) & (n <= m))
            def _(m=m):
                ffn(m, slot)

            lo = m

        copy_w(w2v, w2_sem, w2a, w2b, e, False)
        lo = 0
        for m in SIZES:
            @pl.when((n > lo) & (n <= m))
            def _(m=m):
                down(m)

            lo = m

        @pl.when(e + 1 < experts)
        def _():
            copy_w(w2v, w2_sem, w2a, w2b, e + 1, True)

        @pl.loop(0, (n + UNROLL - 1) // UNROLL)
        def _(g):
            s0 = pl.multiple_of(g * UNROLL, UNROLL)
            for first in range(0, UNROLL, BATCH):
                sums = []
                for i in range(first, first + BATCH):
                    base = pl.multiple_of(tok[e, s0 + i] * chunks, chunks)
                    row = xf[pl.ds(s0 + i, chunks, stride=STRIDE), :]
                    sums.append((base, acc[pl.ds(base, chunks), :] + gate[e, s0 + i] * row))
                for base, val in sums:
                    acc[pl.ds(base, chunks), :] = val

    blk = stage.shape[1]
    n_out = tokens // blk

    @pl.loop(0, n_out)
    def _(i):
        slot = lax.rem(i, 2)
        rows = pl.ds(pl.multiple_of(i * blk, blk), blk)

        @pl.when(i >= 2)
        def _():
            pltpu.make_async_copy(stage.at[slot], out_hbm.at[rows], out_sem.at[slot]).wait()

        for j in range(chunks):
            v = acc[pl.ds(i * (blk * chunks) + j, blk, stride=chunks), :]
            stage[slot, :, j * LANES:(j + 1) * LANES] = v.astype(stage.dtype)
        pltpu.make_async_copy(stage.at[slot], out_hbm.at[rows], out_sem.at[slot]).start()

    for i in range(max(0, n_out - 2), n_out):
        pltpu.make_async_copy(stage.at[i % 2], out_hbm.at[pl.ds(i * blk, blk)], out_sem.at[i % 2]).wait()


def expert_bank(tok, gate, cnt, x3, w_own, w_peer, out_dtype):
    half, chunks, _ = x3[0].shape
    tokens = 2 * half
    per_dev, width, ff = w_own[0].shape
    blk = 128
    anys = pl.BlockSpec(memory_space=pl.ANY)
    smem = pl.BlockSpec(memory_space=pltpu.SMEM)
    flops = 2 * per_dev * 200 * 6 * width * ff
    return pl.pallas_call(
        bank_kernel,
        out_shape=jax.ShapeDtypeStruct((tokens, width), out_dtype),
        in_specs=[smem] * 3 + [anys] * 8,
        out_specs=anys,
        scratch_shapes=[
            pltpu.VMEM((tokens, chunks, LANES), jnp.bfloat16),
            pltpu.VMEM(((tokens + 16) * chunks, LANES), jnp.float32),
            pltpu.VMEM((2, width, ff), jnp.bfloat16),
            pltpu.VMEM((2, width, ff), jnp.bfloat16),
            pltpu.VMEM((ff, width), jnp.bfloat16),
            pltpu.VMEM((chunks * STRIDE, LANES), jnp.float32),
            pltpu.VMEM((CAP, width), jnp.bfloat16),
            pltpu.VMEM((CAP, ff), jnp.bfloat16),
            pltpu.VMEM((2, blk, width), out_dtype),
            pltpu.SemaphoreType.DMA((2,)),
            pltpu.SemaphoreType.DMA((2,)),
            pltpu.SemaphoreType.DMA((2,)),
            pltpu.SemaphoreType.DMA,
            pltpu.SemaphoreType.DMA((2,)),
        ],
        compiler_params=pltpu.CompilerParams(vmem_limit_bytes=66_000_000),
        cost_estimate=pl.CostEstimate(flops=flops, bytes_accessed=6 * per_dev * width * ff * 2, transcendentals=0),
    )(tok, gate, cnt, *x3, *w_own, *w_peer)


def solution(mesh):
    groups = mesh.shape["ep"]
    tok_spec = P(("dp", "ep"), None)
    bank_spec = P("ep", None, None)

    def swap(a, s):
        return lax.ppermute(a, "ep", [(i, i ^ s) for i in range(groups)])

    def device_fn(hidden, w_router, w_gate, w_up, w_down, shared_gate, shared_up, shared_down, top_idx, keep_mask):
        tokens, _ = top_idx.shape
        width = hidden.shape[1]
        experts = w_router.shape[1]
        per_chip = 2 * w_gate.shape[0]
        me = lax.axis_index("ep")
        rows = tokens // 2
        x0 = tuple(hidden[i * rows:(i + 1) * rows].reshape(rows, width // LANES, LANES) for i in range(2))
        x2, x4 = (tuple(swap(h, s) for h in x0) for s in (2, 4))
        w_own = (w_gate, w_up, w_down)
        w_peer = tuple(swap(w, 1) for w in w_own)

        logits = jnp.dot(hidden, w_router, preferred_element_type=jnp.float32)
        prob = ROUTE_SCALE * jax.nn.softmax(logits, axis=-1)
        kept_id = jnp.where(keep_mask > 0, top_idx, experts)
        member = jnp.any(kept_id[:, :, None] == jnp.arange(experts)[None, None, :], axis=1)
        member_b = member.astype(jnp.bfloat16)
        t_ids = jnp.arange(tokens, dtype=jnp.int32)
        before = (t_ids[:, None] > t_ids[None, :]).astype(jnp.bfloat16)
        rank = jnp.dot(before, member_b, preferred_element_type=jnp.float32).astype(jnp.int32)
        rank = jnp.where(member, rank, -1)
        hit = rank[:, :, None] == jnp.arange(CAP, dtype=jnp.int32)[None, None, :]
        slot_tok = jnp.min(jnp.where(hit, t_ids[:, None, None].astype(jnp.float32), float(tokens)), axis=0)
        slot_gate = jnp.sum(jnp.where(hit, prob[:, :, None], 0.0), axis=0)
        lists = jnp.stack([slot_tok, slot_gate], axis=1)

        def lists_of(dev):
            return lax.dynamic_slice_in_dim(lists, (dev // 2) * per_chip, per_chip, axis=0)

        def run(x3, lst, out_dtype):
            own_first = lax.rem(me, 2) == 0
            half = per_chip // 2
            lst = jnp.where(own_first, lst, jnp.concatenate([lst[half:], lst[:half]], axis=0))
            tok = lst[:, 0].astype(jnp.int32)
            cnt = jnp.sum((tok < tokens).astype(jnp.int32), axis=1)
            return expert_bank(tok, lst[:, 1], cnt, x3, w_own, w_peer, out_dtype)

        l_in = {s: swap(lists_of(me ^ s), s) for s in (2, 4, 6)}
        shared = swiglu(hidden, shared_gate, shared_up, shared_down)
        x2, x4, shared, l_in = lax.optimization_barrier((x2, x4, shared, l_in))
        x6 = swap(x4[0], 2), swap(x2[1], 4)
        part2 = run(x2, l_in[2], jnp.bfloat16)
        part4 = run(x4, l_in[4], jnp.bfloat16)
        back2, back4 = swap(part2, 2), swap(part4, 4)
        x6, part4 = lax.optimization_barrier((x6, part4))
        back6 = swap(run(x6, l_in[6], jnp.bfloat16), 6)
        total = shared + run(x0, lists_of(me), jnp.float32)
        for b in (back2, back4, back6):
            total = total + b.astype(jnp.float32)
        return total.astype(jnp.bfloat16)

    return jax.shard_map(device_fn, mesh=mesh, in_specs=(tok_spec, P(), bank_spec, bank_spec, bank_spec, P(), P(), P(), tok_spec, tok_spec), out_specs=tok_spec, check_vma=False)
```

```python
import jax
import jax.numpy as jnp
from jax import lax
from jax.experimental import pallas as pl
from jax.experimental.pallas import tpu as pltpu
from jax.sharding import PartitionSpec as P

ROUTE_SCALE = 16.0
CAP = 384
LANES = 128
STRIDE = CAP + 4
SIZES = (64, 128, 192, 256, 320, 384)
UNROLL = 16
BATCH = 8


def swiglu(tok_rows, gate_w, up_w, down_w):
    h_gate = jnp.dot(tok_rows, gate_w, preferred_element_type=jnp.float32)
    h_up = jnp.dot(tok_rows, up_w, preferred_element_type=jnp.float32)
    act_rows = (jax.nn.silu(h_gate) * h_up).astype(jnp.bfloat16)
    return jnp.dot(act_rows, down_w, preferred_element_type=jnp.float32)


def bank_kernel(tok, gate, cnt, xa_hbm, xb_hbm, w1a, w3a, w2a, w1b, w3b, w2b, out_hbm,
                x_v, acc, w1v, w3v, w2v, xf, xs, hv, stage, x_sem, w1_sem, w3_sem, w2_sem, out_sem):
    _, chunks, _ = x_v.shape
    tokens = out_hbm.shape[0]
    width = chunks * LANES
    per_dev = w1a.shape[0]
    ff = w1a.shape[2]
    experts = 2 * per_dev

    def copy_w(dst, sem, a, b, e, start):
        @pl.when((e < per_dev) & (cnt[e] > 0))
        def _():
            c = pltpu.make_async_copy(a.at[jnp.minimum(e, per_dev - 1)], dst, sem)
            c.start() if start else c.wait()

        @pl.when((e >= per_dev) & (cnt[e] > 0))
        def _():
            c = pltpu.make_async_copy(b.at[jnp.maximum(e - per_dev, 0)], dst, sem)
            c.start() if start else c.wait()

    def in_copies(e, slot, start):
        copy_w(w1v.at[slot], w1_sem.at[slot], w1a, w1b, e, start)
        copy_w(w3v.at[slot], w3_sem.at[slot], w3a, w3b, e, start)

    half = tokens // 2
    x_copies = [pltpu.make_async_copy(src, x_v.at[pl.ds(i * half, half)], x_sem.at[i]) for i, src in enumerate((xa_hbm, xb_hbm))]
    for c in x_copies:
        c.start()
    in_copies(jnp.int32(0), 0, True)
    copy_w(w2v, w2_sem, w2a, w2b, jnp.int32(0), True)

    rows0 = acc.shape[0]
    zblk = 256

    @pl.loop(0, rows0 // zblk)
    def _(i):
        acc[pl.ds(pl.multiple_of(i * zblk, zblk), zblk), :] = jnp.zeros((zblk, LANES), jnp.float32)

    for c in x_copies:
        c.wait()

    def ffn(m, slot):
        for j in range(chunks):
            xs[0:m, j * LANES:(j + 1) * LANES] = xf[j * STRIDE:j * STRIDE + m, :].astype(jnp.bfloat16)

        def gate_up(c0, cw):
            xv = xs[0:m, :]
            g = jnp.dot(xv, w1v[slot, :, c0:c0 + cw], preferred_element_type=jnp.float32)
            u = jnp.dot(xv, w3v[slot, :, c0:c0 + cw], preferred_element_type=jnp.float32)
            hv[0:m, c0:c0 + cw] = (jax.nn.silu(g) * u).astype(jnp.bfloat16)

        for c0 in range(0, ff, 768):
            gate_up(c0, min(768, ff - c0))

    def down(m):
        cols = 1024

        @pl.loop(0, width // cols)
        def _(c):
            o = jnp.dot(hv[0:m, :], w2v[:, pl.ds(pl.multiple_of(c * cols, cols), cols)], preferred_element_type=jnp.float32)
            o = o.astype(jnp.bfloat16).astype(jnp.float32)
            base = c * (cols // LANES * STRIDE)
            for j in range(cols // LANES):
                xf[pl.ds(base + j * STRIDE, m), :] = o[:, j * LANES:(j + 1) * LANES]

    @pl.loop(0, experts)
    def _(e):
        slot = lax.rem(e, 2)
        n = cnt[e]
        first_pair = e * CAP

        @pl.when(e + 1 < experts)
        def _():
            in_copies(e + 1, 1 - slot, True)

        @pl.loop(0, (n + UNROLL - 1) // UNROLL)
        def _(g):
            s0 = pl.multiple_of(g * UNROLL, UNROLL)
            for i in range(UNROLL):
                xf[pl.ds(s0 + i, chunks, stride=STRIDE), :] = x_v[tok[first_pair + s0 + i]].astype(jnp.float32)

        in_copies(e, slot, False)
        lo = 0
        for m in SIZES:
            @pl.when((n > lo) & (n <= m))
            def _(m=m):
                ffn(m, slot)

            lo = m

        copy_w(w2v, w2_sem, w2a, w2b, e, False)
        lo = 0
        for m in SIZES:
            @pl.when((n > lo) & (n <= m))
            def _(m=m):
                down(m)

            lo = m

        @pl.when(e + 1 < experts)
        def _():
            copy_w(w2v, w2_sem, w2a, w2b, e + 1, True)

        @pl.loop(0, (n + UNROLL - 1) // UNROLL)
        def _(g):
            s0 = pl.multiple_of(g * UNROLL, UNROLL)
            for b in range(0, UNROLL, BATCH):
                sums = []
                for i in range(b, b + BATCH):
                    base = pl.multiple_of(tok[first_pair + s0 + i] * chunks, chunks)
                    row = xf[pl.ds(s0 + i, chunks, stride=STRIDE), :]
                    sums.append((base, acc[pl.ds(base, chunks), :] + gate[first_pair + s0 + i] * row))
                for base, val in sums:
                    acc[pl.ds(base, chunks), :] = val

    blk = stage.shape[1]
    n_out = tokens // blk

    @pl.loop(0, n_out)
    def _(i):
        slot = lax.rem(i, 2)
        rows = pl.ds(pl.multiple_of(i * blk, blk), blk)

        @pl.when(i >= 2)
        def _():
            pltpu.make_async_copy(stage.at[slot], out_hbm.at[rows], out_sem.at[slot]).wait()

        for j in range(chunks):
            v = acc[pl.ds(i * (blk * chunks) + j, blk, stride=chunks), :]
            stage[slot, :, j * LANES:(j + 1) * LANES] = v.astype(stage.dtype)
        pltpu.make_async_copy(stage.at[slot], out_hbm.at[rows], out_sem.at[slot]).start()

    for i in range(max(0, n_out - 2), n_out):
        pltpu.make_async_copy(stage.at[i % 2], out_hbm.at[pl.ds(i * blk, blk)], out_sem.at[i % 2]).wait()


def expert_bank(tok, gate, cnt, x3, w_own, w_peer, out_dtype):
    half, chunks, _ = x3[0].shape
    tokens = 2 * half
    per_dev, width, ff = w_own[0].shape
    blk = 128
    anys = pl.BlockSpec(memory_space=pl.ANY)
    smem = pl.BlockSpec(memory_space=pltpu.SMEM)
    flops = 2 * per_dev * 200 * 6 * width * ff
    return pl.pallas_call(
        bank_kernel,
        out_shape=jax.ShapeDtypeStruct((tokens, width), out_dtype),
        in_specs=[smem] * 3 + [anys] * 8,
        out_specs=anys,
        scratch_shapes=[
            pltpu.VMEM((tokens + 8, chunks, LANES), jnp.bfloat16),
            pltpu.VMEM(((tokens + 16) * chunks, LANES), jnp.float32),
            pltpu.VMEM((2, width, ff), jnp.bfloat16),
            pltpu.VMEM((2, width, ff), jnp.bfloat16),
            pltpu.VMEM((ff, width), jnp.bfloat16),
            pltpu.VMEM((chunks * STRIDE, LANES), jnp.float32),
            pltpu.VMEM((CAP, width), jnp.bfloat16),
            pltpu.VMEM((CAP, ff), jnp.bfloat16),
            pltpu.VMEM((2, blk, width), out_dtype),
            pltpu.SemaphoreType.DMA((2,)),
            pltpu.SemaphoreType.DMA((2,)),
            pltpu.SemaphoreType.DMA((2,)),
            pltpu.SemaphoreType.DMA,
            pltpu.SemaphoreType.DMA((2,)),
        ],
        compiler_params=pltpu.CompilerParams(vmem_limit_bytes=66_000_000),
        cost_estimate=pl.CostEstimate(flops=flops, bytes_accessed=6 * per_dev * width * ff * 2, transcendentals=0),
    )(tok.reshape(-1), gate.reshape(-1), cnt, *x3, *w_own, *w_peer)


def solution(mesh):
    groups = mesh.shape["ep"]
    tok_spec = P(("dp", "ep"), None)
    bank_spec = P("ep", None, None)

    def swap(a, s):
        return lax.ppermute(a, "ep", [(i, i ^ s) for i in range(groups)])

    def device_fn(hidden, w_router, w_gate, w_up, w_down, shared_gate, shared_up, shared_down, top_idx, keep_mask):
        tokens, _ = top_idx.shape
        width = hidden.shape[1]
        experts = w_router.shape[1]
        per_chip = 2 * w_gate.shape[0]
        me = lax.axis_index("ep")
        rows = tokens // 2
        x0 = tuple(hidden[i * rows:(i + 1) * rows].reshape(rows, width // LANES, LANES) for i in range(2))
        x2, x4 = (tuple(swap(h, s) for h in x0) for s in (2, 4))
        w_own = (w_gate, w_up, w_down)
        w_peer = tuple(swap(w, 1) for w in w_own)

        logits = jnp.dot(hidden, w_router, preferred_element_type=jnp.float32)
        prob = ROUTE_SCALE * jax.nn.softmax(logits, axis=-1)
        kept_id = jnp.where(keep_mask > 0, top_idx, experts)
        member = jnp.any(kept_id[:, :, None] == jnp.arange(experts)[None, None, :], axis=1)
        member_b = member.astype(jnp.bfloat16)
        t_ids = jnp.arange(tokens, dtype=jnp.int32)
        before = (t_ids[:, None] > t_ids[None, :]).astype(jnp.bfloat16)
        rank = jnp.dot(before, member_b, preferred_element_type=jnp.float32).astype(jnp.int32)
        rank = jnp.where(member, rank, -1)
        hit = rank[:, :, None] == jnp.arange(CAP, dtype=jnp.int32)[None, None, :]
        slot_tok = jnp.min(jnp.where(hit, t_ids[:, None, None].astype(jnp.float32), float(tokens)), axis=0)
        slot_gate = jnp.sum(jnp.where(hit, prob[:, :, None], 0.0), axis=0)
        lists = jnp.stack([slot_tok, slot_gate], axis=1)

        def lists_of(dev):
            return lax.dynamic_slice_in_dim(lists, (dev // 2) * per_chip, per_chip, axis=0)

        def run(x3, lst, out_dtype):
            own_first = lax.rem(me, 2) == 0
            half = per_chip // 2
            lst = jnp.where(own_first, lst, jnp.concatenate([lst[half:], lst[:half]], axis=0))
            tok = lst[:, 0].astype(jnp.int32)
            cnt = jnp.sum((tok < tokens).astype(jnp.int32), axis=1)
            return expert_bank(tok, lst[:, 1], cnt, x3, w_own, w_peer, out_dtype)

        l_in = {s: swap(lists_of(me ^ s), s) for s in (2, 4, 6)}
        shared = swiglu(hidden, shared_gate, shared_up, shared_down)
        x2, x4, shared, l_in = lax.optimization_barrier((x2, x4, shared, l_in))
        x6 = swap(x4[0], 2), swap(x2[1], 4)
        part2 = run(x2, l_in[2], jnp.bfloat16)
        part4 = run(x4, l_in[4], jnp.bfloat16)
        back2, back4 = swap(part2, 2), swap(part4, 4)
        x6, part4 = lax.optimization_barrier((x6, part4))
        back6 = swap(run(x6, l_in[6], jnp.bfloat16), 6)
        total = shared + run(x0, lists_of(me), jnp.float32)
        for b in (back2, back4):
            total = total + b.astype(jnp.float32)
        total, back6 = lax.optimization_barrier((total, back6))
        total = total + back6.astype(jnp.float32)
        return total.astype(jnp.bfloat16)

    return jax.shard_map(device_fn, mesh=mesh, in_specs=(tok_spec, P(), bank_spec, bank_spec, bank_spec, P(), P(), P(), tok_spec, tok_spec), out_specs=tok_spec, check_vma=False)
```

```python
import jax
import jax.numpy as jnp
from jax import lax
from jax.experimental import pallas as pl
from jax.experimental.pallas import tpu as pltpu
from jax.sharding import PartitionSpec as P

ROUTE_SCALE = 16.0
CAP = 384
LANES = 128
STRIDE = CAP + 20
SIZES = (64, 128, 192, 256, 320, 384)
UNROLL = 16
BATCH = 8


def swiglu(tok_rows, gate_w, up_w, down_w):
    h_gate = jnp.dot(tok_rows, gate_w, preferred_element_type=jnp.float32)
    h_up = jnp.dot(tok_rows, up_w, preferred_element_type=jnp.float32)
    act_rows = (jax.nn.silu(h_gate) * h_up).astype(jnp.bfloat16)
    return jnp.dot(act_rows, down_w, preferred_element_type=jnp.float32)


def bank_kernel(tok, gate, cnt, xa_hbm, xb_hbm, w1a, w3a, w2a, w1b, w3b, w2b, outa_hbm, outb_hbm,
                x_v, acc, w1v, w3v, w2v, xf, xs, hv, stage, x_sem, w1_sem, w3_sem, w2_sem, out_sem):
    _, chunks, _ = x_v.shape
    tokens = 2 * outa_hbm.shape[0]
    width = chunks * LANES
    per_dev = w1a.shape[0]
    ff = w1a.shape[2]
    experts = 2 * per_dev

    def copy_w(dst, sem, a, b, e, start):
        @pl.when((e < per_dev) & (cnt[2 * e] + cnt[2 * e + 1] > 0))
        def _():
            c = pltpu.make_async_copy(a.at[jnp.minimum(e, per_dev - 1)], dst, sem)
            c.start() if start else c.wait()

        @pl.when((e >= per_dev) & (cnt[2 * e] + cnt[2 * e + 1] > 0))
        def _():
            c = pltpu.make_async_copy(b.at[jnp.maximum(e - per_dev, 0)], dst, sem)
            c.start() if start else c.wait()

    def in_copies(e, slot, start):
        copy_w(w1v.at[slot], w1_sem.at[slot], w1a, w1b, e, start)
        copy_w(w3v.at[slot], w3_sem.at[slot], w3a, w3b, e, start)

    half = tokens // 2
    x_copies = [pltpu.make_async_copy(src, x_v.at[pl.ds(i * half, half)], x_sem.at[i]) for i, src in enumerate((xa_hbm, xb_hbm))]
    for c in x_copies:
        c.start()
    in_copies(jnp.int32(0), 0, True)
    copy_w(w2v, w2_sem, w2a, w2b, jnp.int32(0), True)

    rows0 = acc.shape[0]
    zblk = 256

    @pl.loop(0, rows0 // zblk)
    def _(i):
        acc[pl.ds(pl.multiple_of(i * zblk, zblk), zblk), :] = jnp.zeros((zblk, LANES), jnp.float32)

    for c in x_copies:
        c.wait()

    def ffn(m, slot):
        for j in range(chunks):
            xs[0:m, j * LANES:(j + 1) * LANES] = xf[j * STRIDE:j * STRIDE + m, :].astype(jnp.bfloat16)

        def gate_up(c0, cw):
            xv = xs[0:m, :]
            g = jnp.dot(xv, w1v[slot, :, c0:c0 + cw], preferred_element_type=jnp.float32)
            u = jnp.dot(xv, w3v[slot, :, c0:c0 + cw], preferred_element_type=jnp.float32)
            hv[0:m, c0:c0 + cw] = (jax.nn.silu(g) * u).astype(jnp.bfloat16)

        for c0 in range(0, ff, 768):
            gate_up(c0, min(768, ff - c0))

    def down(m):
        cols = 1024

        @pl.loop(0, width // cols)
        def _(c):
            o = jnp.dot(hv[0:m, :], w2v[:, pl.ds(pl.multiple_of(c * cols, cols), cols)], preferred_element_type=jnp.float32)
            o = o.astype(jnp.bfloat16).astype(jnp.float32)
            base = c * (cols // LANES * STRIDE)
            for j in range(cols // LANES):
                xf[pl.ds(base + j * STRIDE, m), :] = o[:, j * LANES:(j + 1) * LANES]

    @pl.loop(0, experts)
    def _(e):
        slot = lax.rem(e, 2)
        n_seg = (cnt[2 * e], cnt[2 * e + 1])
        both = n_seg[0] + n_seg[1]
        merged = both <= CAP

        @pl.when(e + 1 < experts)
        def _():
            in_copies(e + 1, 1 - slot, True)

        @pl.loop(0, jnp.where(merged, 1, 2))
        def _(p):
            n = jnp.where(merged, both, jnp.where(p == 0, n_seg[0], n_seg[1]))
            counts = [jnp.where(merged | (p == q), n_seg[q], 0) for q in range(2)]
            starts = (0, jnp.where(merged, n_seg[0], 0))

            for q in range(2):
                @pl.loop(0, (counts[q] + UNROLL - 1) // UNROLL)
                def _(g, q=q):
                    pair = (2 * e + q) * CAP + g * UNROLL
                    row = starts[q] + g * UNROLL
                    for i in range(UNROLL):
                        xf[pl.ds(row + i, chunks, stride=STRIDE), :] = x_v[tok[pair + i]].astype(jnp.float32)

            @pl.when(p == 0)
            def _():
                in_copies(e, slot, False)

            lo = 0
            for m in SIZES:
                @pl.when((n > lo) & (n <= m))
                def _(m=m):
                    ffn(m, slot)

                lo = m

            @pl.when(p == 0)
            def _():
                copy_w(w2v, w2_sem, w2a, w2b, e, False)

            lo = 0
            for m in SIZES:
                @pl.when((n > lo) & (n <= m))
                def _(m=m):
                    down(m)

                lo = m

            @pl.when((e + 1 < experts) & (merged | (p == 1)))
            def _():
                copy_w(w2v, w2_sem, w2a, w2b, e + 1, True)

            for q in range(2):
                @pl.loop(0, (counts[q] + UNROLL - 1) // UNROLL)
                def _(g, q=q):
                    pair = (2 * e + q) * CAP + g * UNROLL
                    first = starts[q] + g * UNROLL
                    for b in range(0, UNROLL, BATCH):
                        sums = []
                        for i in range(b, b + BATCH):
                            base = pl.multiple_of(tok[pair + i] * chunks, chunks)
                            row = xf[pl.ds(first + i, chunks, stride=STRIDE), :]
                            sums.append((base, acc[pl.ds(base, chunks), :] + gate[pair + i] * row))
                        for base, val in sums:
                            acc[pl.ds(base, chunks), :] = val

    blk = stage.shape[1]
    n_out = half // blk
    for k, out_hbm in enumerate((outa_hbm, outb_hbm)):
        @pl.loop(0, n_out)
        def _(i, k=k, out_hbm=out_hbm):
            slot = lax.rem(i, 2)
            rows = pl.ds(pl.multiple_of(i * blk, blk), blk)

            @pl.when(i >= 2)
            def _():
                pltpu.make_async_copy(stage.at[slot], out_hbm.at[rows], out_sem.at[slot]).wait()

            for j in range(chunks):
                v = acc[pl.ds((k * half + i * blk) * chunks + j, blk, stride=chunks), :]
                stage[slot, :, j * LANES:(j + 1) * LANES] = v.astype(stage.dtype)
            pltpu.make_async_copy(stage.at[slot], out_hbm.at[rows], out_sem.at[slot]).start()

        for i in range(n_out - 2, n_out):
            pltpu.make_async_copy(stage.at[i % 2], out_hbm.at[pl.ds(i * blk, blk)], out_sem.at[i % 2]).wait()


def expert_bank(tok, gate, cnt, x3, w_own, w_peer, out_dtype):
    half, chunks, _ = x3[0].shape
    tokens = 2 * half
    per_dev, width, ff = w_own[0].shape
    blk = 128
    anys = pl.BlockSpec(memory_space=pl.ANY)
    smem = pl.BlockSpec(memory_space=pltpu.SMEM)
    flops = 2 * per_dev * 200 * 6 * width * ff
    return pl.pallas_call(
        bank_kernel,
        out_shape=[jax.ShapeDtypeStruct((half, width), out_dtype)] * 2,
        in_specs=[smem] * 3 + [anys] * 8,
        out_specs=[anys] * 2,
        scratch_shapes=[
            pltpu.VMEM((tokens + 8, chunks, LANES), jnp.bfloat16),
            pltpu.VMEM(((tokens + 16) * chunks, LANES), jnp.float32),
            pltpu.VMEM((2, width, ff), jnp.bfloat16),
            pltpu.VMEM((2, width, ff), jnp.bfloat16),
            pltpu.VMEM((ff, width), jnp.bfloat16),
            pltpu.VMEM((chunks * STRIDE, LANES), jnp.float32),
            pltpu.VMEM((CAP, width), jnp.bfloat16),
            pltpu.VMEM((CAP, ff), jnp.bfloat16),
            pltpu.VMEM((2, blk, width), out_dtype),
            pltpu.SemaphoreType.DMA((2,)),
            pltpu.SemaphoreType.DMA((2,)),
            pltpu.SemaphoreType.DMA((2,)),
            pltpu.SemaphoreType.DMA,
            pltpu.SemaphoreType.DMA((2,)),
        ],
        compiler_params=pltpu.CompilerParams(vmem_limit_bytes=66_000_000),
        cost_estimate=pl.CostEstimate(flops=flops, bytes_accessed=6 * per_dev * width * ff * 2, transcendentals=0),
    )(tok.reshape(-1), gate.reshape(-1), cnt, *x3, *w_own, *w_peer)


def join_kernel(shared, *refs):
    out = refs[-1]
    sums = []
    for h in range(2):
        total = refs[h][...].astype(jnp.float32)
        for r in refs[2 + h:-1:2]:
            total = total + r[...].astype(jnp.float32)
        sums.append(total)
    for g in range(out.shape[0] // 16):
        pair = jnp.concatenate([t[g * 8:g * 8 + 8] for t in sums], axis=0)
        out[g * 16:g * 16 + 16, :] = (shared[g * 16:g * 16 + 16, :] + pair).astype(out.dtype)


def join(shared, parts):
    tokens, width = shared.shape
    blk = 128
    half_spec = pl.BlockSpec((blk // 2, width), lambda i: (i, 0))
    full_spec = pl.BlockSpec((blk, width), lambda i: (i, 0))
    return pl.pallas_call(
        join_kernel,
        out_shape=jax.ShapeDtypeStruct((tokens, width), jnp.bfloat16),
        grid=(tokens // blk,),
        in_specs=[full_spec] + [half_spec] * len(parts),
        out_specs=full_spec,
        cost_estimate=pl.CostEstimate(flops=8 * tokens * width, bytes_accessed=14 * tokens * width, transcendentals=0),
    )(shared, *parts)


def solution(mesh):
    groups = mesh.shape["ep"]
    tok_spec = P(("dp", "ep"), None)
    bank_spec = P("ep", None, None)

    def swap(a, s):
        return lax.ppermute(a, "ep", [(i, i ^ s) for i in range(groups)])

    def device_fn(hidden, w_router, w_gate, w_up, w_down, shared_gate, shared_up, shared_down, top_idx, keep_mask):
        tokens, _ = top_idx.shape
        width = hidden.shape[1]
        experts = w_router.shape[1]
        per_chip = 2 * w_gate.shape[0]
        me = lax.axis_index("ep")
        rows = tokens // 2

        def halves(a):
            tiles = a.reshape(tokens // 16, 2, 8, a.shape[1])
            return tuple(tiles[:, h].reshape(rows, a.shape[1]) for h in range(2))

        x0 = tuple(h.reshape(rows, width // LANES, LANES) for h in halves(hidden))
        x2, x4 = (tuple(swap(h, s) for h in x0) for s in (2, 4))
        w_own = (w_gate, w_up, w_down)
        w_peer = tuple(swap(w, 1) for w in w_own)

        logits = jnp.dot(hidden, w_router, preferred_element_type=jnp.float32)
        prob = ROUTE_SCALE * jax.nn.softmax(logits, axis=-1)
        kept_id = jnp.where(keep_mask > 0, top_idx, experts)
        member = jnp.any(kept_id[:, :, None] == jnp.arange(experts)[None, None, :], axis=1)
        prob = jnp.concatenate(halves(prob), axis=1)
        member = jnp.concatenate(halves(member.astype(jnp.bfloat16)), axis=1)
        t_ids = jnp.arange(rows, dtype=jnp.int32)
        before = (t_ids[:, None] > t_ids[None, :]).astype(jnp.bfloat16)
        rank = jnp.dot(before, member, preferred_element_type=jnp.float32).astype(jnp.int32)
        rank = jnp.where(member > 0, rank, -1)
        hit = rank[:, :, None] == jnp.arange(CAP, dtype=jnp.int32)[None, None, :]
        slot_tok = jnp.min(jnp.where(hit, t_ids[:, None, None].astype(jnp.float32), float(rows)), axis=0)
        slot_gate = jnp.sum(jnp.where(hit, prob[:, :, None], 0.0), axis=0)
        lists = jnp.stack([slot_tok, slot_gate], axis=1).reshape(2, experts, 2, CAP)

        def lists_of(dev):
            return lax.dynamic_slice_in_dim(lists, (dev // 2) * per_chip, per_chip, axis=1)

        def run(xs, lst, out_dtype):
            half = per_chip // 2
            lst = jnp.stack(lst, axis=1)
            lst = jnp.where(lax.rem(me, 2) == 0, lst, jnp.concatenate([lst[half:], lst[:half]], axis=0))
            tok = lst[:, :, 0].astype(jnp.int32)
            used = tok < rows
            cnt = jnp.sum(used.astype(jnp.int32), axis=2).reshape(-1)
            tok = jnp.where(used, tok + jnp.array([0, rows], jnp.int32)[None, :, None], tokens)
            return expert_bank(tok, lst[:, :, 1], cnt, xs, w_own, w_peer, out_dtype)

        l_in = {s: swap(lists_of(me ^ s), s) for s in (2, 4, 6)}
        shared = swiglu(hidden, shared_gate, shared_up, shared_down)
        x2, x4, shared, l_in = lax.optimization_barrier((x2, x4, shared, l_in))
        x6 = swap(x4[0], 2), swap(x2[1], 4)
        a2, a4 = run((x2[0], x4[0]), (l_in[2][0], l_in[4][0]), jnp.bfloat16)
        back_a = swap(a2, 2), swap(a4, 4)
        x6, a2 = lax.optimization_barrier((x6, a2))
        b0, b1 = run(x6, (l_in[6][0], l_in[6][1]), jnp.bfloat16)
        back_b = swap(b0, 6), swap(b1, 6)
        c2, c4 = run((x2[1], x4[1]), (l_in[2][1], l_in[4][1]), jnp.bfloat16)
        back_c = swap(c2, 2), swap(c4, 4)
        mine = lists_of(me)
        own = run(x0, (mine[0], mine[1]), jnp.bfloat16)
        parts = [*own, *back_b, back_a[0], back_c[0], back_a[1], back_c[1]]
        return join(shared, parts)

    return jax.shard_map(device_fn, mesh=mesh, in_specs=(tok_spec, P(), bank_spec, bank_spec, bank_spec, P(), P(), P(), tok_spec, tok_spec), out_specs=tok_spec, check_vma=False)
```
